32 devices in a mesh: rep: 2 (over y), seq: 8 (over z, x), head: 2 (over core).
Axes of the slice: x: 2, y: 2, z: 4, core: 2. Of those that a mesh axis runs over, the one named last changes fastest.
Arguments:
- prompt_query: bfloat16 [2048, 1792], P(('rep', 'seq', 'head')), parts along dimension 0, may hold values from -12 to 12
- prompt_key: bfloat16 [2048, 256], P(('rep', 'seq', 'head')), parts along dimension 0, may hold values from -12 to 12
- prompt_value: bfloat16 [2048, 256], P(('rep', 'seq', 'head')), parts along dimension 0, may hold values from -24 to 24
- prompt_length: int32 [2], P('rep'), parts along dimension 0, may hold values from 512 to 1024
- span_order: int32 [32], P('rep'), parts along dimension 0, may hold values from 0 to 15, each once
- new_query: bfloat16 [32, 1792], P('rep', 'head'), parts along dimension 0, may hold values from -12 to 12
- new_key: bfloat16 [32, 256], P('rep', 'head'), parts along dimension 0, may hold values from -12 to 12
- new_value: bfloat16 [32, 256], P('rep', 'head'), parts along dimension 0, may hold values from -24 to 24
- cache_key: bfloat16 [32, 2, 2048, 128], P('rep', 'head', 'seq'), parts along dimension 0, may hold values from -12 to 12
- cache_value: bfloat16 [32, 2, 2048, 128], P('rep', 'head', 'seq'), parts along dimension 0, may hold values from -24 to 24
- cache_length: int32 [32], P('rep'), parts along dimension 0, may hold values from 1280 to 2048
Outputs:
- prompt_attended: bfloat16 [2048, 1792], P(('rep', 'seq', 'head')), parts along dimension 0
- decode_attended: bfloat16 [32, 1792], P('rep', 'head'), parts along dimension 0
The draws below stay inside these ranges and needn't reach their ends.
There are 2 independent parts, one for each index of `rep`. The reference program is written for one: setup_inputs(seed, part) draws one part's arguments, and reference() takes and returns one part's arrays. A program takes and returns all parts, laid end to end along the dimension named above; each array names one. Nothing has to cross between parts.
Inputs may be any that keep to these rules, and one draw needn't show every extreme that they name: `span_order`: each of the 16 spans stands once.
All inputs are finite; a program needn't handle non-finite values.
Results may differ from the reference program's by a relative error of at most 0.0045.
Values may be sent and summed in bfloat16 or wider, within the bound.
No kernel may reach another device: no remote copies, remote signals or barrier semaphores. Data moves between devices by JAX's collectives and lax.ppermute only.
A program may use at most 128 MiB of HBM per device.

```python
import math
import jax
import jax.numpy as jnp
from jax import lax

HD = 128
QH = 14
KVH = 2
SPAN = 64
SESS = 16
CTX_DEV = 256
NCHUNK = 16
PROMPT = 1024
CTX = 2048


def prompt_fields(key):
    query_key = jax.random.fold_in(key, 31)
    keys_key = jax.random.fold_in(key, 32)
    broad_key = jax.random.fold_in(key, 34)
    row_ids = jnp.arange(PROMPT, dtype=jnp.int32)
    queries = 1.2 * jnp.clip(jax.random.normal(query_key, (PROMPT, QH * HD), jnp.float32), -6.0, 6.0)
    broad = jax.random.uniform(broad_key, (PROMPT, QH * HD), jnp.float32, -6.0, 6.0)
    broad_rows = row_ids % 64 == 5
    queries = jnp.where(broad_rows[:, None], broad, queries)
    keys_drawn = 1.2 * jnp.clip(jax.random.normal(keys_key, (PROMPT, KVH * HD), jnp.float32), -6.0, 6.0)
    return (queries, keys_drawn)


def decode_fields(key):
    query_key = jax.random.fold_in(key, 41)
    keys_key = jax.random.fold_in(key, 42)
    broad_key = jax.random.fold_in(key, 44)
    session_ids = jnp.arange(SESS, dtype=jnp.int32)
    queries = 1.2 * jnp.clip(jax.random.normal(query_key, (SESS, QH * HD), jnp.float32), -6.0, 6.0)
    broad = jax.random.uniform(broad_key, (SESS, QH * HD), jnp.float32, -6.0, 6.0)
    broad_rows = session_ids % 4 == 1
    queries = jnp.where(broad_rows[:, None], broad, queries)
    keys_drawn = 1.2 * jnp.clip(jax.random.normal(keys_key, (SESS, KVH, CTX, HD), jnp.float32), -6.0, 6.0)
    far_slot = CTX // 2 + CTX_DEV // 2
    planted_scale = 5.0 / (1.44 * math.sqrt(HD))
    leading = queries.reshape(SESS, KVH, QH // KVH, HD)[:, :, 0, :]
    keys_drawn = keys_drawn.at[:, :, far_slot, :].set(planted_scale * leading)
    return (queries, keys_drawn)


def draw_prompt_query(key, part):
    return prompt_fields(key)[0].astype(jnp.bfloat16)


def draw_prompt_key(key, part):
    return prompt_fields(key)[1].astype(jnp.bfloat16)


def draw_new_query(key, part):
    return decode_fields(key)[0].astype(jnp.bfloat16)


def draw_cache_key(key, part):
    return decode_fields(key)[1].astype(jnp.bfloat16)


def plant(values, key, low, top_value):
    longest = values.shape.index(max(values.shape))
    spots = []
    for shift in (0, 1):
        where = [jax.random.randint(jax.random.fold_in(key, axis), (), 0, length) for axis, length in enumerate(values.shape)]
        where[longest] = (where[longest] + shift) % values.shape[longest]
        spots.append(tuple(where))
    return values.at[spots[0]].set(low).at[spots[1]].set(top_value)


def level_of(key, shape, split, least, high):
    factor_of = 1.0
    for position, shards_of in split:
        draws = jax.random.uniform(jax.random.fold_in(jax.random.fold_in(key, 6), position), (shards_of,), jnp.float32, least / len(split), high / len(split))
        factor_of = factor_of * jnp.repeat(jnp.exp(draws), shape[position] // shards_of).reshape((-1,) + (1,) * (len(shape) - 1 - position))
    return factor_of


def scatter_about(key, shape, width, most, shards=(), kind=jnp.bfloat16):
    values = jax.random.normal(key, shape, jnp.float32) * width
    if len(shards) > 0:
        values = level_of(key, shape, shards, -0.22, 0.18) * values
    return jnp.clip(values, min=-most, max=most).astype(kind)


def setup_inputs(seed: int = 0, part: int = 0) -> dict:
    keys = jax.random.split(jax.random.key(seed), 12)
    part_splits = jax.random.split(jax.random.fold_in(keys[11], part), 12)
    return {
        "prompt_query": draw_prompt_query(jax.random.fold_in(jax.random.fold_in(keys[11], part), 71), part),
        "prompt_key": draw_prompt_key(jax.random.fold_in(jax.random.fold_in(keys[11], part), 71), part),
        "prompt_value": scatter_about(part_splits[2], (PROMPT, KVH * HD), 4.0, 24.0, ((0, 16),)),
        "prompt_length": jax.random.randint(part_splits[3], (1,), PROMPT // 2, PROMPT + 1).astype(jnp.int32),
        "span_order": jax.random.permutation(part_splits[4], NCHUNK).astype(jnp.int32),
        "new_query": draw_new_query(jax.random.fold_in(jax.random.fold_in(keys[11], part), 71), part),
        "new_key": scatter_about(part_splits[6], (SESS, KVH * HD), 2.0, 12.0, ((1, 2),)),
        "new_value": scatter_about(part_splits[7], (SESS, KVH * HD), 4.0, 24.0, ((1, 2),)),
        "cache_key": draw_cache_key(jax.random.fold_in(jax.random.fold_in(keys[11], part), 71), part),
        "cache_value": scatter_about(part_splits[9], (SESS, KVH, CTX, HD), 4.0, 24.0, ((1, 2), (2, 8))),
        "cache_length": plant(jax.random.randint(part_splits[10], (SESS,), CTX // 2 + CTX_DEV, CTX + 1), jax.random.fold_in(part_splits[10], 1), CTX // 2 + CTX_DEV, CTX).astype(jnp.int32),
    }


def reference(prompt_query, prompt_key, prompt_value, prompt_length, span_order, new_query, new_key, new_value, cache_key, cache_value, cache_length):
    head_group = QH // KVH
    score_scale = 1.0 / math.sqrt(HD)
    row_ids = jnp.arange(PROMPT, dtype=jnp.int32)
    positions = (span_order[row_ids // SPAN] * SPAN + row_ids % SPAN).astype(jnp.int32)
    length_limit = prompt_length[0]
    key_table = prompt_key.astype(jnp.float32).reshape(PROMPT, KVH, HD)
    value_table = prompt_value.astype(jnp.float32).reshape(PROMPT, KVH, HD)
    key_live = positions < length_limit
    block_rows = math.gcd(PROMPT, 256)

    def one_block(block_index):
        start_row = (block_index * block_rows).astype(jnp.int32)
        queries = lax.dynamic_slice_in_dim(prompt_query, start_row, block_rows, 0).astype(jnp.float32)
        queries = queries.reshape(block_rows, KVH, head_group, HD)
        query_pos = lax.dynamic_slice_in_dim(positions, start_row, block_rows, 0)
        scores = jnp.einsum('rkgd,nkd->kgrn', queries, key_table) * score_scale
        allowed = (positions[None, :] <= query_pos[:, None]) & key_live[None, :]
        scores = jnp.where(allowed, scores, -1e+30)
        row_max = lax.optimization_barrier(jnp.max(scores, axis=-1, keepdims=True))
        weights = jnp.where(allowed, jnp.exp(scores - row_max), 0.0)
        row_total = lax.optimization_barrier(jnp.sum(weights, axis=-1))
        rounded = lax.optimization_barrier(weights.astype(jnp.bfloat16)).astype(jnp.float32)
        weighted = jnp.einsum('kgrn,nkd->rkgd', rounded, value_table)
        result = weighted / jnp.transpose(row_total, (2, 0, 1))[..., None]
        result = jnp.where((query_pos < length_limit)[:, None, None, None], result, 0.0)
        return result.reshape(block_rows, QH * HD).astype(jnp.bfloat16)
    prompt_attended = lax.map(one_block, jnp.arange(PROMPT // block_rows, dtype=jnp.int32)).reshape(PROMPT, QH * HD)
    cache_pos = jnp.arange(CTX, dtype=jnp.int32)

    def one_session(session):
        queries = new_query[session].astype(jnp.float32).reshape(KVH, head_group, HD)
        keys_here = cache_key[session].astype(jnp.float32)
        values_here = cache_value[session].astype(jnp.float32)
        fresh_key = new_key[session].astype(jnp.float32).reshape(KVH, HD)
        fresh_value = new_value[session].astype(jnp.float32).reshape(KVH, HD)
        valid = cache_pos < cache_length[session]
        scores = jnp.einsum('kgd,ktd->kgt', queries, keys_here) * score_scale
        scores = jnp.where(valid[None, None, :], scores, -1e+30)
        own_score = jnp.einsum('kgd,kd->kg', queries, fresh_key) * score_scale
        row_max = jnp.maximum(lax.optimization_barrier(jnp.max(scores, axis=-1)), own_score)
        weights = jnp.where(valid[None, None, :], jnp.exp(scores - row_max[..., None]), 0.0)
        own_weight = jnp.exp(own_score - row_max)
        row_total = lax.optimization_barrier(jnp.sum(weights, axis=-1)) + own_weight
        rounded = lax.optimization_barrier(weights.astype(jnp.bfloat16)).astype(jnp.float32)
        own_rounded = lax.optimization_barrier(own_weight.astype(jnp.bfloat16)).astype(jnp.float32)
        weighted = jnp.einsum('kgt,ktd->kgd', rounded, values_here) + own_rounded[..., None] * fresh_value[:, None, :]
        return (weighted / row_total[..., None]).reshape(QH * HD).astype(jnp.bfloat16)
    decode_attended = lax.map(one_session, jnp.arange(SESS, dtype=jnp.int32))
    return (prompt_attended, decode_attended)
```

```python
import functools
import math

import jax
import jax.numpy as jnp
from jax import lax
from jax.experimental import pallas as pl
from jax.experimental.pallas import tpu as pltpu
from jax.sharding import PartitionSpec as P

HD = 128
QH = 14
KVH = 2
NEG = -1e30
STAT = 3


def split3(x):
    hi = x.astype(jnp.bfloat16)
    rest = x - hi.astype(jnp.float32)
    mid = rest.astype(jnp.bfloat16)
    low = (rest - mid.astype(jnp.float32)).astype(jnp.bfloat16)
    return hi, mid, low


def join3(ref, at):
    return (
        ref[at].astype(jnp.float32) + ref[at + 1].astype(jnp.float32)
    ) + ref[at + 2].astype(jnp.float32)


def decode_kernel(meta, lens, q_ref, nk_ref, nv_ref, k_ref, v_ref, out_ref, q_scr, o_scr, l_scr, n_scr):
    step = pl.program_id(0)
    sessions, group, ctx = q_ref.shape[0], q_ref.shape[1] // HD, k_ref.shape[2]
    per_step = k_ref.shape[0]
    scale = math.log2(math.e) / math.sqrt(HD)

    @pl.when(step == 0)
    def _():
        n_scr[0] = nk_ref[...].astype(jnp.float32)
        n_scr[1] = nv_ref[...].astype(jnp.float32)
        for h in range(q_scr.shape[0]):
            if h < group:
                q_scr[h] = q_ref[:, h * HD : (h + 1) * HD].astype(jnp.float32)
            else:
                q_scr[h] = jnp.zeros((sessions, HD), jnp.float32)

    first = meta[0]
    owner = meta[1]
    cols = lax.broadcasted_iota(jnp.int32, (q_scr.shape[0], ctx), 1)
    for i in range(per_step):
        s = step * per_step + i
        q = q_scr[:, pl.ds(s, 1), :].reshape(q_scr.shape[0], HD)
        qb = q.astype(jnp.bfloat16)
        score = (
            lax.dot_general(
                qb, k_ref[i, 0], (((1,), (1,)), ((), ())), preferred_element_type=jnp.float32
            )
            * scale
        )
        valid = cols + first < lens[s]
        score = jnp.where(valid, score, NEG)
        nk = n_scr[0, pl.ds(s, 1), :]
        nv = n_scr[1, pl.ds(s, 1), :]
        own = jnp.sum(q * nk, axis=1, keepdims=True) * scale
        own = jnp.where(owner > 0, own, NEG)
        top = jnp.maximum(jnp.max(score, axis=1, keepdims=True), own)
        weight = jnp.where(valid, jnp.exp2(score - top), 0.0)
        own_w = jnp.where(owner > 0, jnp.exp2(own - top), 0.0)
        total = jnp.sum(weight, axis=1, keepdims=True) + own_w
        acc = jnp.dot(weight.astype(jnp.bfloat16), v_ref[i, 0], preferred_element_type=jnp.float32)
        acc = acc + own_w.astype(jnp.bfloat16).astype(jnp.float32) * nv
        live = total > 0.0
        safe = jnp.where(live, total, 1.0)
        o_scr[:, pl.ds(s, 1), :] = (acc / safe).reshape(q_scr.shape[0], 1, HD)
        lse = jnp.where(live, top + jnp.log2(safe), NEG)
        l_scr[:, pl.ds(s, 1), :] = jnp.broadcast_to(lse, (q_scr.shape[0], HD)).reshape(
            q_scr.shape[0], 1, HD
        )

    @pl.when(step == pl.num_programs(0) - 1)
    def _():
        lane = lax.broadcasted_iota(jnp.int32, (sessions, HD), 1)
        stat = jnp.zeros((sessions, HD), jnp.float32)
        for h in range(group):
            out_ref[h] = o_scr[h].astype(jnp.bfloat16)
            stat = jnp.where(lane == h, l_scr[h], stat)
        for j, part in enumerate(split3(stat)):
            out_ref[group + j] = part


def decode_local(meta, lens, query, new_key, new_value, cache_key, cache_value):
    sessions, width = query.shape
    group = width // HD
    ctx = cache_key.shape[2]
    per_step = max(n for n in (1, 2, 4) if sessions % n == 0)
    padded = -(-group // 8) * 8
    whole = pl.BlockSpec(query.shape, lambda i, *_: (0, 0))
    fresh = pl.BlockSpec(new_key.shape, lambda i, *_: (0, 0))
    cache = pl.BlockSpec((per_step, 1, ctx, HD), lambda i, *_: (i, 0, 0, 0))
    return pl.pallas_call(
        decode_kernel,
        grid_spec=pltpu.PrefetchScalarGridSpec(
            num_scalar_prefetch=2,
            grid=(sessions // per_step,),
            in_specs=[whole, fresh, fresh, cache, cache],
            out_specs=pl.BlockSpec((group + STAT, sessions, HD), lambda i, *_: (0, 0, 0)),
            scratch_shapes=[pltpu.VMEM((padded, sessions, HD), jnp.float32)] * 3
            + [pltpu.VMEM((2, sessions, HD), jnp.float32)],
        ),
        out_shape=jax.ShapeDtypeStruct((group + STAT, sessions, HD), jnp.bfloat16),
        cost_estimate=pl.CostEstimate(
            flops=2_000_000_000, bytes_accessed=cache_key.size * 4, transcendentals=0
        ),
        name="decode_local",
    )(meta, lens, query, new_key, new_value, cache_key, cache_value)


def merge_kernel(a_ref, b_ref, out_ref, *, final):
    group = a_ref.shape[0] - STAT
    la = join3(a_ref, group)
    lb = join3(b_ref, group)
    top = jnp.maximum(la, lb)
    ea = jnp.exp2(la - top)
    eb = jnp.exp2(lb - top)
    total = ea + eb
    wa = ea / total
    wb = eb / total
    for h in range(group):
        out = a_ref[h].astype(jnp.float32) * wa[:, h : h + 1] + b_ref[h].astype(
            jnp.float32
        ) * wb[:, h : h + 1]
        if final:
            out_ref[:, h * HD : (h + 1) * HD] = out.astype(jnp.bfloat16)
        else:
            out_ref[h] = out.astype(jnp.bfloat16)
    if not final:
        for j, part in enumerate(split3(top + jnp.log2(total))):
            out_ref[group + j] = part


def merge(a, b, final):
    rows, sessions, _ = a.shape
    shape = (sessions, (rows - STAT) * HD) if final else a.shape
    return pl.pallas_call(
        functools.partial(merge_kernel, final=final),
        out_shape=jax.ShapeDtypeStruct(shape, jnp.bfloat16),
        name="decode_merge",
    )(a, b)


def attend_kernel(meta, q_ref, pos_ref, kv_ref, *refs, first, last):
    if first:
        state_in, refs = None, refs
    else:
        state_in, refs = refs[:3], refs[3:]
    if last:
        out_ref, acc_s, m_s, l_s = refs
    else:
        acc_s, m_s, l_s = refs
    step = pl.program_id(0)
    rows = q_ref.shape[0]
    group = QH // KVH
    scale = math.log2(math.e) / math.sqrt(HD)

    @pl.when(step == 0)
    def _():
        if first:
            acc_s[...] = jnp.zeros(acc_s.shape, jnp.float32)
            m_s[...] = jnp.full(m_s.shape, NEG, jnp.float32)
            l_s[...] = jnp.zeros(l_s.shape, jnp.float32)
        else:
            acc_s[...] = state_in[0][...]
            m_s[...] = state_in[1][...]
            l_s[...] = state_in[2][...]

    q_pos = meta[0] + lax.broadcasted_iota(jnp.int32, (rows, 1), 0)
    limit = jnp.minimum(q_pos, meta[1] - 1)
    allowed = pos_ref[...] <= limit
    allowed = jnp.concatenate([allowed.astype(jnp.float32)] * group, axis=0) > 0.0
    for g in range(KVH):
        q = jnp.concatenate(
            [q_ref[:, (g * group + h) * HD : (g * group + h + 1) * HD] for h in range(group)], axis=0
        )
        key = kv_ref[:, g * HD : (g + 1) * HD]
        value = kv_ref[:, (KVH + g) * HD : (KVH + g + 1) * HD]
        score = (
            lax.dot_general(q, key, (((1,), (1,)), ((), ())), preferred_element_type=jnp.float32)
            * scale
        )
        score = jnp.where(allowed, score, NEG)
        m_old = m_s[g]
        m_new = jnp.maximum(m_old, jnp.max(score, axis=1, keepdims=True))
        weight = jnp.where(allowed, jnp.exp2(score - m_new[:, :1]), 0.0)
        factor = jnp.exp2(m_old - m_new)
        total = l_s[g] * factor + jnp.sum(weight, axis=1, keepdims=True)
        acc = acc_s[g] * factor + jnp.dot(
            weight.astype(jnp.bfloat16), value, preferred_element_type=jnp.float32
        )
        acc_s[g] = acc
        m_s[g] = m_new
        l_s[g] = total

    if last:

        @pl.when(step == pl.num_programs(0) - 1)
        def _():
            live = q_pos < meta[1]
            for g in range(KVH):
                for h in range(group):
                    part = slice(h * rows, (h + 1) * rows)
                    out = acc_s[g, part] / l_s[g, part]
                    at = (g * group + h) * HD
                    out_ref[:, at : at + HD] = jnp.where(live, out, 0.0).astype(jnp.bfloat16)


def attend(meta, query, pos, kv, state, last):
    rows = query.shape[0]
    group = QH // KVH
    keys = kv.shape[0]
    block = math.gcd(keys, 512)
    first = state is None
    shape = (KVH, group * rows, HD)
    full = pl.BlockSpec(shape, lambda i, *_: (0, 0, 0))
    sds = jax.ShapeDtypeStruct(shape, jnp.float32)
    specs = [
        pl.BlockSpec(query.shape, lambda i, *_: (0, 0)),
        pl.BlockSpec((1, block), lambda i, *_: (0, i)),
        pl.BlockSpec((block, kv.shape[1]), lambda i, *_: (i, 0)),
    ] + ([] if first else [full] * 3)
    return pl.pallas_call(
        functools.partial(attend_kernel, first=first, last=last),
        grid_spec=pltpu.PrefetchScalarGridSpec(
            num_scalar_prefetch=1,
            grid=(keys // block,),
            in_specs=specs,
            out_specs=pl.BlockSpec(query.shape, lambda i, *_: (0, 0)) if last else [full] * 3,
            scratch_shapes=[pltpu.VMEM(shape, jnp.float32)] * 3 if last else [],
        ),
        out_shape=jax.ShapeDtypeStruct(query.shape, jnp.bfloat16) if last else [sds] * 3,
        cost_estimate=pl.CostEstimate(
            flops=4_000_000_000, bytes_accessed=kv.size * 2, transcendentals=0
        ),
        name="attend",
    )(meta, query, pos, kv, *(() if first else state))


def per_device(
    prompt_query,
    prompt_key,
    prompt_value,
    prompt_length,
    span_order,
    new_query,
    new_key,
    new_value,
    cache_key,
    cache_value,
    cache_length,
):
    seq, head = lax.axis_size("seq"), lax.axis_size("head")
    count = seq * head
    span_rows = prompt_query.shape[0]
    seq_id = lax.axis_index("seq")
    me = seq_id * head + lax.axis_index("head")
    bits = [1 << b for b in reversed(range(seq.bit_length() - 1))]

    def swap(x, bit):
        return lax.ppermute(x, "seq", [(i, i ^ bit) for i in range(seq)])

    masks = [0]
    for bit in bits:
        masks = masks + [m ^ (bit * head) for m in masks]
    masks = masks + [m ^ 1 for m in masks]
    pick = jnp.arange(count, dtype=jnp.int32)
    source = me ^ jnp.asarray(masks, jnp.int32)
    spans = jnp.sum(jnp.where(source[:, None] == pick[None, :], span_order[None, :], 0), axis=1)
    pos = (spans[:, None] * span_rows + jnp.arange(span_rows, dtype=jnp.int32)[None, :]).reshape(1, -1)
    meta = jnp.stack([spans[0] * span_rows, prompt_length[0]])

    local_ctx = cache_key.shape[2]
    dec_meta = jnp.stack([seq_id * local_ctx, (seq_id == 0).astype(jnp.int32)])
    dec = decode_local(
        dec_meta, cache_length, new_query, new_key, new_value, cache_key, cache_value
    )

    kv = jnp.concatenate([prompt_key, prompt_value], axis=1)
    state = None
    for n, bit in enumerate(bits):
        other = swap(kv, bit)
        if n == len(bits) - 1:
            half = kv.shape[0]
            state = attend(meta, prompt_query, pos[:, :half], kv, None, False)
            state = attend(meta, prompt_query, pos[:, half : 2 * half], other, state, False)
        kv = jnp.concatenate([kv, other], axis=0)
    half = kv.shape[0]
    other = lax.ppermute(kv, "head", [(i, i ^ 1) for i in range(head)])
    prompt_attended = attend(meta, prompt_query, pos[:, half:], other, state, True)

    order = bits[1:] + bits[:1]
    for n, bit in enumerate(order):
        dec = merge(dec, swap(dec, bit), n == len(order) - 1)
    return (prompt_attended, dec)


def solution(mesh):
    return jax.shard_map(
        per_device,
        mesh=mesh,
        in_specs=(
            P(("rep", "seq", "head"), None),
            P(("rep", "seq", "head"), None),
            P(("rep", "seq", "head"), None),
            P("rep"),
            P("rep"),
            P("rep", "head"),
            P("rep", "head"),
            P("rep", "head"),
            P("rep", "head", "seq", None),
            P("rep", "head", "seq", None),
            P("rep"),
        ),
        out_specs=(P(("rep", "seq", "head"), None), P("rep", "head")),
        check_vma=False,
    )
```

```python
import functools
import math

import jax
import jax.numpy as jnp
from jax import lax
from jax.experimental import pallas as pl
from jax.experimental.pallas import tpu as pltpu
from jax.sharding import PartitionSpec as P

HD = 128
QH = 14
KVH = 2
NEG = -1e30
STAT = 3


def split3(x):
    hi = x.astype(jnp.bfloat16)
    rest = x - hi.astype(jnp.float32)
    mid = rest.astype(jnp.bfloat16)
    low = (rest - mid.astype(jnp.float32)).astype(jnp.bfloat16)
    return hi, mid, low


def join3(ref, at):
    return (
        ref[at].astype(jnp.float32) + ref[at + 1].astype(jnp.float32)
    ) + ref[at + 2].astype(jnp.float32)


def vmem(x):
    if x.size * x.dtype.itemsize > 1 << 20:
        return x
    return pltpu.with_memory_space_constraint(x, pltpu.VMEM)


def in_vmem():
    return pl.BlockSpec(memory_space=pltpu.VMEM)


def in_smem():
    return pl.BlockSpec(memory_space=pltpu.SMEM)


def decode_kernel(lens, q_ref, nk_ref, nv_ref, k_ref, v_ref, out_ref, q_scr, o_scr, l_scr, n_scr):
    step = pl.program_id(0)
    sessions, group, ctx = q_ref.shape[0], q_ref.shape[1] // HD, k_ref.shape[2]
    per_step = k_ref.shape[0]
    padded = q_scr.shape[0]
    scale = math.log2(math.e) / math.sqrt(HD)
    seq_id = lax.axis_index("seq")
    first = seq_id * ctx
    owner = jnp.full((1, 1), seq_id, jnp.int32) == 0

    @pl.when(step == 0)
    def _():
        n_scr[0] = nk_ref[...].astype(jnp.float32)
        n_scr[1] = nv_ref[...].astype(jnp.float32)
        for h in range(padded):
            if h < group:
                q_scr[h] = q_ref[:, h * HD : (h + 1) * HD].astype(jnp.float32)
            else:
                q_scr[h] = jnp.zeros((sessions, HD), jnp.float32)

    cols = lax.broadcasted_iota(jnp.int32, (padded, ctx), 1)
    scores, valids, owns, fresh = [], [], [], []
    for i in range(per_step):
        s = step * per_step + i
        q = q_scr[:, pl.ds(s, 1), :].reshape(padded, HD)
        scores.append(
            lax.dot_general(
                q.astype(jnp.bfloat16),
                k_ref[i, 0],
                (((1,), (1,)), ((), ())),
                preferred_element_type=jnp.float32,
            )
        )
        valids.append((cols < lens[s] - first).astype(jnp.float32))
        owns.append(q * n_scr[0, pl.ds(s, 1), :])
        fresh.append(jnp.broadcast_to(n_scr[1, pl.ds(s, 1), :], (padded, HD)))
    valid = jnp.concatenate(valids, axis=0) > 0.0
    score = jnp.where(valid, jnp.concatenate(scores, axis=0) * scale, NEG)
    own = jnp.sum(jnp.concatenate(owns, axis=0), axis=1, keepdims=True) * scale
    own = jnp.where(owner, own, NEG)
    top = jnp.maximum(jnp.max(score, axis=1, keepdims=True), own)
    weight = jnp.where(valid, jnp.exp2(score - top), 0.0)
    own_w = jnp.where(owner, jnp.exp2(own - top), 0.0)
    total = jnp.sum(weight, axis=1, keepdims=True) + own_w
    weight = weight.astype(jnp.bfloat16)
    acc = jnp.concatenate(
        [
            jnp.dot(
                weight[i * padded : (i + 1) * padded],
                v_ref[i, 0],
                preferred_element_type=jnp.float32,
            )
            for i in range(per_step)
        ],
        axis=0,
    )
    acc = acc + own_w.astype(jnp.bfloat16).astype(jnp.float32) * jnp.concatenate(fresh, axis=0)
    live = total > 0.0
    safe = jnp.where(live, total, 1.0)
    out = acc / safe
    lse = jnp.broadcast_to(jnp.where(live, top + jnp.log2(safe), NEG), out.shape)
    for i in range(per_step):
        s = step * per_step + i
        part = slice(i * padded, (i + 1) * padded)
        o_scr[:, pl.ds(s, 1), :] = out[part].reshape(padded, 1, HD)
        l_scr[:, pl.ds(s, 1), :] = lse[part].reshape(padded, 1, HD)

    @pl.when(step == pl.num_programs(0) - 1)
    def _():
        lane = lax.broadcasted_iota(jnp.int32, (sessions, HD), 1)
        stat = jnp.zeros((sessions, HD), jnp.float32)
        for h in range(group):
            out_ref[h] = o_scr[h].astype(jnp.bfloat16)
            stat = jnp.where(lane == h, l_scr[h], stat)
        for j, part in enumerate(split3(stat)):
            out_ref[group + j] = part


def decode_local(lens, query, new_key, new_value, cache_key, cache_value):
    sessions, width = query.shape
    group = width // HD
    ctx = cache_key.shape[2]
    per_step = max(n for n in (1, 2, 4) if sessions % n == 0)
    padded = -(-group // 8) * 8
    cache = pl.BlockSpec((per_step, 1, ctx, HD), lambda i: (i, 0, 0, 0))
    return pl.pallas_call(
        decode_kernel,
        grid=(sessions // per_step,),
        in_specs=[in_smem(), in_vmem(), in_vmem(), in_vmem(), cache, cache],
        out_specs=in_vmem(),
        scratch_shapes=[pltpu.VMEM((padded, sessions, HD), jnp.float32)] * 3
        + [pltpu.VMEM((2, sessions, HD), jnp.float32)],
        out_shape=pltpu.VMEM((group + STAT, sessions, HD), jnp.bfloat16),
        cost_estimate=pl.CostEstimate(
            flops=2_000_000_000, bytes_accessed=cache_key.size * 4, transcendentals=0
        ),
        name="decode_local",
    )(lens, vmem(query), vmem(new_key), vmem(new_value), cache_key, cache_value)


def merge_kernel(a_ref, b_ref, out_ref, *, final):
    group = a_ref.shape[0] - STAT
    la = join3(a_ref, group)
    lb = join3(b_ref, group)
    top = jnp.maximum(la, lb)
    ea = jnp.exp2(la - top)
    eb = jnp.exp2(lb - top)
    total = ea + eb
    wa = ea / total
    wb = eb / total
    for h in range(group):
        out = a_ref[h].astype(jnp.float32) * wa[:, h : h + 1] + b_ref[h].astype(
            jnp.float32
        ) * wb[:, h : h + 1]
        if final:
            out_ref[:, h * HD : (h + 1) * HD] = out.astype(jnp.bfloat16)
        else:
            out_ref[h] = out.astype(jnp.bfloat16)
    if not final:
        for j, part in enumerate(split3(top + jnp.log2(total))):
            out_ref[group + j] = part


def merge(a, b, final):
    rows, sessions, _ = a.shape
    shape = (sessions, (rows - STAT) * HD) if final else a.shape
    return pl.pallas_call(
        functools.partial(merge_kernel, final=final),
        in_specs=[in_vmem(), in_vmem()],
        out_specs=in_vmem(),
        out_shape=jax.ShapeDtypeStruct(shape, jnp.bfloat16)
        if final
        else pltpu.VMEM(shape, jnp.bfloat16),
        name="decode_merge",
    )(vmem(a), vmem(b))


def attend_kernel(span_ref, len_ref, q_ref, *refs, bases, bits, first, last):
    kv_refs, refs = refs[: len(bases)], refs[len(bases) :]
    if not first:
        state_in, refs = refs[:3], refs[3:]
    rows = q_ref.shape[0]
    group = QH // KVH
    scale = math.log2(math.e) / math.sqrt(HD)
    me = lax.axis_index("seq") * lax.axis_size("head") + lax.axis_index("head")
    length = len_ref[0]
    q_pos = span_ref[me] * rows + lax.broadcasted_iota(jnp.int32, (rows, 1), 0)
    limit = jnp.minimum(q_pos, length - 1)
    keys = kv_refs[0].shape[0]
    block = math.gcd(keys, 256)
    chunks = block // rows
    state = []
    for g in range(KVH):
        if first:
            shape = (group * rows, HD)
            state.append(
                (
                    jnp.zeros(shape, jnp.float32),
                    jnp.full((group * rows, 1), NEG, jnp.float32),
                    jnp.zeros((group * rows, 1), jnp.float32),
                )
            )
        else:
            state.append((state_in[0][g], state_in[1][g][:, :1], state_in[2][g][:, :1]))
    queries = [
        jnp.concatenate(
            [q_ref[:, (g * group + h) * HD : (g * group + h + 1) * HD] for h in range(group)], axis=0
        )
        for g in range(KVH)
    ]

    def positions(b, base):
        lane = lax.broadcasted_iota(jnp.int32, (1, block), 1)
        pos = lane
        for c in range(chunks):
            at = b * chunks + c
            source = me ^ base
            for t, bit in enumerate(bits):
                source = source ^ (((at >> t) & 1) * bit)
            start = (span_ref[source] - c) * rows
            inside = (lane >= c * rows) & (lane < (c + 1) * rows)
            pos = jnp.where(inside, lane + start, pos)
        return pos

    def advance(state, parts):
        allowed = jnp.concatenate(
            [(pos <= limit).astype(jnp.float32) for _, _, pos in parts], axis=1
        )
        allowed = jnp.concatenate([allowed] * group, axis=0) > 0.0
        result = []
        for g in range(KVH):
            acc, m_old, total = state[g]
            score = jnp.concatenate(
                [
                    lax.dot_general(
                        queries[g],
                        ref[at, g * HD : (g + 1) * HD],
                        (((1,), (1,)), ((), ())),
                        preferred_element_type=jnp.float32,
                    )
                    for ref, at, _ in parts
                ],
                axis=1,
            )
            score = jnp.where(allowed, score * scale, NEG)
            m_new = jnp.maximum(m_old, jnp.max(score, axis=1, keepdims=True))
            weight = jnp.where(allowed, jnp.exp2(score - m_new), 0.0)
            factor = jnp.exp2(m_old - m_new)
            total = total * factor + jnp.sum(weight, axis=1, keepdims=True)
            weight = weight.astype(jnp.bfloat16)
            acc = acc * factor
            for n, (ref, at, _) in enumerate(parts):
                acc = acc + jnp.dot(
                    weight[:, n * block : (n + 1) * block],
                    ref[at, (KVH + g) * HD : (KVH + g + 1) * HD],
                    preferred_element_type=jnp.float32,
                )
            result.append((acc, m_new, total))
        return result

    if keys == block:
        at = slice(0, block)
        state = advance(state, [(r, at, positions(0, base)) for r, base in zip(kv_refs, bases)])
    else:

        def body(b, state):
            at = pl.ds(pl.multiple_of(b * block, block), block)
            return advance(state, [(r, at, positions(b, base)) for r, base in zip(kv_refs, bases)])

        state = lax.fori_loop(0, keys // block, body, state)

    if last:
        live = q_pos < length
        for g in range(KVH):
            acc, _, total = state[g]
            out = acc / total
            for h in range(group):
                at = (g * group + h) * HD
                part = out[h * rows : (h + 1) * rows]
                refs[0][:, at : at + HD] = jnp.where(live, part, 0.0).astype(jnp.bfloat16)
    else:
        for g in range(KVH):
            for ref, value in zip(refs, state[g]):
                ref[g] = jnp.broadcast_to(value, ref.shape[1:])


def attend(spans, length, query, pieces, bases, bits, state, last):
    rows = query.shape[0]
    first = state is None
    shape = (KVH, QH // KVH * rows, HD)
    operands = [query, *pieces] + ([] if first else list(state))
    return pl.pallas_call(
        functools.partial(attend_kernel, bases=bases, bits=bits, first=first, last=last),
        in_specs=[in_smem(), in_smem()] + [in_vmem()] * len(operands),
        out_specs=in_vmem() if last else [in_vmem()] * 3,
        out_shape=jax.ShapeDtypeStruct(query.shape, jnp.bfloat16)
        if last
        else [pltpu.VMEM(shape, jnp.float32)] * 3,
        cost_estimate=pl.CostEstimate(
            flops=4_000_000_000, bytes_accessed=query.size * 2, transcendentals=0
        ),
        name="attend",
    )(spans, length, *(vmem(x) for x in operands[: 1 + len(pieces)]), *operands[1 + len(pieces) :])


def per_device(
    prompt_query,
    prompt_key,
    prompt_value,
    prompt_length,
    span_order,
    new_query,
    new_key,
    new_value,
    cache_key,
    cache_value,
    cache_length,
):
    seq, head = lax.axis_size("seq"), lax.axis_size("head")
    bits = [1 << b for b in reversed(range(seq.bit_length() - 1))]

    def swap(x, bit):
        return lax.ppermute(x, "seq", [(i, i ^ bit) for i in range(seq)])

    def partner(x):
        return lax.ppermute(x, "head", [(i, i ^ 1) for i in range(head)])

    kv = jnp.concatenate([prompt_key, prompt_value], axis=1)
    other = swap(kv, bits[0])
    dec = decode_local(
        cache_length, new_query, new_key, new_value, cache_key, cache_value
    )
    kv = jnp.concatenate([kv, other], axis=0)
    for bit in bits[1:-1]:
        other = swap(kv, bit)
        kv = jnp.concatenate([kv, other], axis=0)
    masks = [bit * head for bit in bits[:-1]]
    far = bits[-1] * head
    kv_far = swap(kv, bits[-1])
    kv_pair = partner(kv)
    state = attend(
        span_order, prompt_length, prompt_query, [kv, kv_pair], (0, 1), masks, None, False
    )
    kv_far_pair = partner(kv_far)
    prompt_attended = attend(
        span_order,
        prompt_length,
        prompt_query,
        [kv_far, kv_far_pair],
        (far, far ^ 1),
        masks,
        state,
        True,
    )

    order = bits[1:] + bits[:1]
    for n, bit in enumerate(order):
        other = swap(dec, bit)
        dec = merge(dec, other, n == len(order) - 1)
    return (prompt_attended, dec)


def solution(mesh):
    return jax.shard_map(
        per_device,
        mesh=mesh,
        in_specs=(
            P(("rep", "seq", "head"), None),
            P(("rep", "seq", "head"), None),
            P(("rep", "seq", "head"), None),
            P("rep"),
            P("rep"),
            P("rep", "head"),
            P("rep", "head"),
            P("rep", "head"),
            P("rep", "head", "seq", None),
            P("rep", "head", "seq", None),
            P("rep"),
        ),
        out_specs=(P(("rep", "seq", "head"), None), P("rep", "head")),
        check_vma=False,
    )
```

```python
import functools
import math

import jax
import jax.numpy as jnp
from jax import lax
from jax.experimental import pallas as pl
from jax.experimental.pallas import tpu as pltpu
from jax.sharding import PartitionSpec as P

HD = 128
QH = 14
KVH = 2
NEG = -1e30
STAT = 3


def split3(x):
    hi = x.astype(jnp.bfloat16)
    rest = x - hi.astype(jnp.float32)
    mid = rest.astype(jnp.bfloat16)
    low = (rest - mid.astype(jnp.float32)).astype(jnp.bfloat16)
    return hi, mid, low


def join3(ref, at):
    return (
        ref[at].astype(jnp.float32) + ref[at + 1].astype(jnp.float32)
    ) + ref[at + 2].astype(jnp.float32)


def vmem(x):
    if x.size * x.dtype.itemsize > 1 << 20:
        return x
    return pltpu.with_memory_space_constraint(x, pltpu.VMEM)


def in_vmem():
    return pl.BlockSpec(memory_space=pltpu.VMEM)


def in_smem():
    return pl.BlockSpec(memory_space=pltpu.SMEM)


def decode_kernel(lens, q_ref, nk_ref, nv_ref, k_ref, v_ref, out_ref, q_scr, o_scr, l_scr, n_scr):
    step = pl.program_id(0)
    sessions, group, ctx = q_ref.shape[0], q_ref.shape[1] // HD, k_ref.shape[2]
    per_step = k_ref.shape[0]
    padded = q_scr.shape[0]
    scale = math.log2(math.e) / math.sqrt(HD)
    seq_id = lax.axis_index("seq")
    first = seq_id * ctx
    owner = jnp.full((1, 1), seq_id, jnp.int32) == 0

    @pl.when(step == 0)
    def _():
        n_scr[0] = nk_ref[...].astype(jnp.float32)
        n_scr[1] = nv_ref[...].astype(jnp.float32)
        for h in range(padded):
            if h < group:
                q_scr[h] = q_ref[:, h * HD : (h + 1) * HD].astype(jnp.float32)
            else:
                q_scr[h] = jnp.zeros((sessions, HD), jnp.float32)

    cols = lax.broadcasted_iota(jnp.int32, (padded, ctx), 1)
    scores, valids, owns, fresh = [], [], [], []
    for i in range(per_step):
        s = step * per_step + i
        q = q_scr[:, pl.ds(s, 1), :].reshape(padded, HD)
        scores.append(
            lax.dot_general(
                q.astype(jnp.bfloat16),
                k_ref[i, 0],
                (((1,), (1,)), ((), ())),
                preferred_element_type=jnp.float32,
            )
        )
        valids.append((cols < lens[s] - first).astype(jnp.float32))
        owns.append(q * n_scr[0, pl.ds(s, 1), :])
        fresh.append(jnp.broadcast_to(n_scr[1, pl.ds(s, 1), :], (padded, HD)))
    valid = jnp.concatenate(valids, axis=0) > 0.0
    score = jnp.where(valid, jnp.concatenate(scores, axis=0) * scale, NEG)
    own = jnp.sum(jnp.concatenate(owns, axis=0), axis=1, keepdims=True) * scale
    own = jnp.where(owner, own, NEG)
    top = jnp.maximum(jnp.max(score, axis=1, keepdims=True), own)
    weight = jnp.where(valid, jnp.exp2(score - top), 0.0)
    own_w = jnp.where(owner, jnp.exp2(own - top), 0.0)
    total = jnp.sum(weight, axis=1, keepdims=True) + own_w
    weight = weight.astype(jnp.bfloat16)
    acc = jnp.concatenate(
        [
            jnp.dot(
                weight[i * padded : (i + 1) * padded],
                v_ref[i, 0],
                preferred_element_type=jnp.float32,
            )
            for i in range(per_step)
        ],
        axis=0,
    )
    acc = acc + own_w.astype(jnp.bfloat16).astype(jnp.float32) * jnp.concatenate(fresh, axis=0)
    live = total > 0.0
    safe = jnp.where(live, total, 1.0)
    out = acc / safe
    lse = jnp.broadcast_to(jnp.where(live, top + jnp.log2(safe), NEG), out.shape)
    for i in range(per_step):
        s = step * per_step + i
        part = slice(i * padded, (i + 1) * padded)
        o_scr[:, pl.ds(s, 1), :] = out[part].reshape(padded, 1, HD)
        l_scr[:, pl.ds(s, 1), :] = lse[part].reshape(padded, 1, HD)

    @pl.when(step == pl.num_programs(0) - 1)
    def _():
        lane = lax.broadcasted_iota(jnp.int32, (sessions, HD), 1)
        stat = jnp.zeros((sessions, HD), jnp.float32)
        for h in range(group):
            out_ref[h] = o_scr[h].astype(jnp.bfloat16)
            stat = jnp.where(lane == h, l_scr[h], stat)
        for j, part in enumerate(split3(stat)):
            out_ref[group + j] = part


def decode_local(lens, query, new_key, new_value, cache_key, cache_value):
    sessions, width = query.shape
    group = width // HD
    ctx = cache_key.shape[2]
    per_step = max(n for n in (1, 2, 4) if sessions % n == 0)
    padded = -(-group // 8) * 8
    cache = pl.BlockSpec((per_step, 1, ctx, HD), lambda i: (i, 0, 0, 0))
    return pl.pallas_call(
        decode_kernel,
        grid=(sessions // per_step,),
        in_specs=[in_smem(), in_vmem(), in_vmem(), in_vmem(), cache, cache],
        out_specs=in_vmem(),
        scratch_shapes=[pltpu.VMEM((padded, sessions, HD), jnp.float32)] * 3
        + [pltpu.VMEM((2, sessions, HD), jnp.float32)],
        out_shape=pltpu.VMEM((group + STAT, sessions, HD), jnp.bfloat16),
        cost_estimate=pl.CostEstimate(
            flops=2_000_000_000, bytes_accessed=cache_key.size * 4, transcendentals=0
        ),
        compiler_params=pltpu.CompilerParams(vmem_limit_bytes=16 << 20),
        name="decode_local",
    )(lens, vmem(query), vmem(new_key), vmem(new_value), cache_key, cache_value)


def merge_kernel(a_ref, b_ref, out_ref, *, final):
    group = a_ref.shape[0] - STAT
    la = join3(a_ref, group)
    lb = join3(b_ref, group)
    top = jnp.maximum(la, lb)
    ea = jnp.exp2(la - top)
    eb = jnp.exp2(lb - top)
    total = ea + eb
    wa = ea / total
    wb = eb / total
    for h in range(group):
        out = a_ref[h].astype(jnp.float32) * wa[:, h : h + 1] + b_ref[h].astype(
            jnp.float32
        ) * wb[:, h : h + 1]
        if final:
            out_ref[:, h * HD : (h + 1) * HD] = out.astype(jnp.bfloat16)
        else:
            out_ref[h] = out.astype(jnp.bfloat16)
    if not final:
        for j, part in enumerate(split3(top + jnp.log2(total))):
            out_ref[group + j] = part


def merge(a, b, final):
    rows, sessions, _ = a.shape
    shape = (sessions, (rows - STAT) * HD) if final else a.shape
    return pl.pallas_call(
        functools.partial(merge_kernel, final=final),
        in_specs=[in_vmem(), in_vmem()],
        out_specs=in_vmem(),
        out_shape=jax.ShapeDtypeStruct(shape, jnp.bfloat16)
        if final
        else pltpu.VMEM(shape, jnp.bfloat16),
        compiler_params=pltpu.CompilerParams(vmem_limit_bytes=8 << 20),
        name="decode_merge",
    )(vmem(a), vmem(b))


def attend_kernel(span_ref, len_ref, q_ref, *refs, bases, bits, first, last):
    kv_refs, refs = refs[: len(bases)], refs[len(bases) :]
    if not first:
        state_in, refs = refs[0], refs[1:]
    rows = q_ref.shape[0]
    group = QH // KVH
    scale = math.log2(math.e) / math.sqrt(HD)
    me = lax.axis_index("seq") * lax.axis_size("head") + lax.axis_index("head")
    length = len_ref[0]
    q_pos = span_ref[me] * rows + lax.broadcasted_iota(jnp.int32, (rows, 1), 0)
    limit = jnp.minimum(q_pos, length - 1)
    keys = kv_refs[0].shape[0]
    block = math.gcd(keys, 256)
    chunks = block // rows
    state = []
    for g in range(KVH):
        if first:
            shape = (group * rows, HD)
            state.append(
                (
                    jnp.zeros(shape, jnp.float32),
                    jnp.full((group * rows, 1), NEG, jnp.float32),
                    jnp.zeros((group * rows, 1), jnp.float32),
                )
            )
        else:
            state.append(
                (state_in[g, :, :HD], state_in[g, :, HD : HD + 1], state_in[g, :, 2 * HD - 1 :])
            )
    queries = [
        jnp.concatenate(
            [q_ref[:, (g * group + h) * HD : (g * group + h + 1) * HD] for h in range(group)], axis=0
        )
        for g in range(KVH)
    ]

    def positions(b, base):
        lane = lax.broadcasted_iota(jnp.int32, (1, block), 1)
        pos = lane
        for c in range(chunks):
            at = b * chunks + c
            source = me ^ base
            for t, bit in enumerate(bits):
                source = source ^ (((at >> t) & 1) * bit)
            start = (span_ref[source] - c) * rows
            inside = (lane >= c * rows) & (lane < (c + 1) * rows)
            pos = jnp.where(inside, lane + start, pos)
        return pos

    def advance(state, parts):
        allowed = jnp.concatenate(
            [(pos <= limit).astype(jnp.float32) for _, _, pos in parts], axis=1
        )
        allowed = jnp.concatenate([allowed] * group, axis=0) > 0.0
        result = []
        for g in range(KVH):
            acc, m_old, total = state[g]
            score = jnp.concatenate(
                [
                    lax.dot_general(
                        queries[g],
                        ref[at, g * HD : (g + 1) * HD],
                        (((1,), (1,)), ((), ())),
                        preferred_element_type=jnp.float32,
                    )
                    for ref, at, _ in parts
                ],
                axis=1,
            )
            score = jnp.where(allowed, score * scale, NEG)
            m_new = jnp.maximum(m_old, jnp.max(score, axis=1, keepdims=True))
            weight = jnp.where(allowed, jnp.exp2(score - m_new), 0.0)
            factor = jnp.exp2(m_old - m_new)
            total = total * factor + jnp.sum(weight, axis=1, keepdims=True)
            weight = weight.astype(jnp.bfloat16)
            acc = acc * factor
            for n, (ref, at, _) in enumerate(parts):
                acc = acc + jnp.dot(
                    weight[:, n * block : (n + 1) * block],
                    ref[at, (KVH + g) * HD : (KVH + g + 1) * HD],
                    preferred_element_type=jnp.float32,
                )
            result.append((acc, m_new, total))
        return result

    if keys == block:
        at = slice(0, block)
        state = advance(state, [(r, at, positions(0, base)) for r, base in zip(kv_refs, bases)])
    else:

        def body(b, state):
            at = pl.ds(pl.multiple_of(b * block, block), block)
            return advance(state, [(r, at, positions(b, base)) for r, base in zip(kv_refs, bases)])

        state = lax.fori_loop(0, keys // block, body, state)

    if last:
        live = q_pos < length
        for g in range(KVH):
            acc, _, total = state[g]
            out = acc / total
            for h in range(group):
                at = (g * group + h) * HD
                part = out[h * rows : (h + 1) * rows]
                refs[0][:, at : at + HD] = jnp.where(live, part, 0.0).astype(jnp.bfloat16)
    else:
        lane = lax.broadcasted_iota(jnp.int32, (group * rows, HD), 1)
        for g in range(KVH):
            acc, top, total = state[g]
            refs[0][g, :, :HD] = acc
            refs[0][g, :, HD:] = jnp.where(lane < HD // 2, top, total)


def attend(spans, length, query, pieces, bases, bits, state, last):
    rows = query.shape[0]
    first = state is None
    shape = (KVH, QH // KVH * rows, 2 * HD)
    operands = [query, *pieces] + ([] if first else [state])
    return pl.pallas_call(
        functools.partial(attend_kernel, bases=bases, bits=bits, first=first, last=last),
        in_specs=[in_smem(), in_smem()] + [in_vmem()] * len(operands),
        out_specs=in_vmem(),
        out_shape=jax.ShapeDtypeStruct(query.shape, jnp.bfloat16)
        if last
        else pltpu.VMEM(shape, jnp.float32),
        cost_estimate=pl.CostEstimate(
            flops=4_000_000_000, bytes_accessed=query.size * 2, transcendentals=0
        ),
        compiler_params=pltpu.CompilerParams(vmem_limit_bytes=32 << 20),
        name="attend",
    )(spans, length, *(vmem(x) for x in operands))


def per_device(
    prompt_query,
    prompt_key,
    prompt_value,
    prompt_length,
    span_order,
    new_query,
    new_key,
    new_value,
    cache_key,
    cache_value,
    cache_length,
):
    seq, head = lax.axis_size("seq"), lax.axis_size("head")
    bits = [1 << b for b in reversed(range(seq.bit_length() - 1))]

    def swap(x, bit):
        return lax.ppermute(x, "seq", [(i, i ^ bit) for i in range(seq)])

    def partner(x):
        return lax.ppermute(x, "head", [(i, i ^ 1) for i in range(head)])

    kv = jnp.concatenate([prompt_key, prompt_value], axis=1)
    other = swap(kv, bits[0])
    dec = decode_local(
        cache_length, new_query, new_key, new_value, cache_key, cache_value
    )
    kv = jnp.concatenate([kv, other], axis=0)
    for bit in bits[1:-1]:
        other = swap(kv, bit)
        kv = jnp.concatenate([kv, other], axis=0)
    masks = [bit * head for bit in bits[:-1]]
    far = bits[-1] * head
    kv_far = swap(kv, bits[-1])
    kv_pair = partner(kv)
    state = attend(
        span_order, prompt_length, prompt_query, [kv, kv_pair], (0, 1), masks, None, False
    )
    kv_far_pair = partner(kv_far)
    prompt_attended = attend(
        span_order,
        prompt_length,
        prompt_query,
        [kv_far, kv_far_pair],
        (far, far ^ 1),
        masks,
        state,
        True,
    )

    order = bits[1:] + bits[:1]
    for n, bit in enumerate(order):
        other = swap(dec, bit)
        dec = merge(dec, other, n == len(order) - 1)
    return (prompt_attended, dec)


def solution(mesh):
    return jax.shard_map(
        per_device,
        mesh=mesh,
        in_specs=(
            P(("rep", "seq", "head"), None),
            P(("rep", "seq", "head"), None),
            P(("rep", "seq", "head"), None),
            P("rep"),
            P("rep"),
            P("rep", "head"),
            P("rep", "head"),
            P("rep", "head"),
            P("rep", "head", "seq", None),
            P("rep", "head", "seq", None),
            P("rep"),
        ),
        out_specs=(P(("rep", "seq", "head"), None), P("rep", "head")),
        check_vma=False,
    )
```
